32 devices in a mesh: rep: 2 (over x), dp: 16 (over y, z, core).
Axes of the slice: x: 2, y: 2, z: 4, core: 2. Of those that a mesh axis runs over, the one named last changes fastest.
Arguments:
- a: bfloat16 [32, 4, 8192, 896], P(('rep', 'dp')), parts along dimension 0
- g: bfloat16 [32, 4, 8192, 2560], P(('rep', 'dp')), parts along dimension 0
Outputs:
- output: bfloat16 [8, 896, 2560], P('rep'), parts along dimension 0
There are 2 independent parts. The reference program is written for one: setup_inputs(seed, part) draws one part's arguments, and reference() takes and returns one part's arrays. A program takes and returns all parts, laid end to end along the dimension named above; each array names one.
All inputs are finite; a program needn't handle non-finite values.
Results may differ from the reference program's by a relative error of at most 0.012.
Values are sent between devices in bfloat16 or wider.
A program may use at most 2 GiB of HBM per device.

```python
import jax
import jax.numpy as jnp
from jax import lax

DEVICES = 16
MATRICES = 4
TOKENS = 8192
D = 896
FF = 2560


def setup_inputs(seed: int = 0, part: int = 0) -> dict:
    ka, kg, ks = (jax.random.fold_in(k, part) for k in jax.random.split(jax.random.key(seed), 3))
    size = 2.0 ** jax.random.uniform(ks, (DEVICES, MATRICES, 1, 1), jnp.float32, -1.0, 1.0)
    a = jax.random.normal(ka, (DEVICES, MATRICES, TOKENS, D), jnp.float32)
    g = size * jax.random.normal(kg, (DEVICES, MATRICES, TOKENS, FF), jnp.float32) * (DEVICES * TOKENS) ** -0.5
    return {"a": a.astype(jnp.bfloat16), "g": g.astype(jnp.bfloat16)}


def reference(a, g):
    def take(so_far, one):
        return so_far + jnp.einsum("ntd,ntf->ndf", *one, preferred_element_type=jnp.float32), None

    return lax.scan(take, jnp.zeros((MATRICES, D, FF), jnp.float32), (a, g))[0].astype(jnp.bfloat16)
```

```python
import jax
import jax.numpy as jnp
from jax import lax
from jax.experimental import pallas as pl
from jax.experimental.pallas import tpu as pltpu
from jax.sharding import PartitionSpec as P

MESH = pl.DeviceIdType.MESH
F32, BF16 = jnp.float32, jnp.bfloat16

COLS = 256
DEPTH = 4096
GBUFS = 3
ASLABS = 8
SLOTS = 4
FSLOTS = 8
LAGS = dict(a1=3, a2t1=5, a2t2=6, a3t1=7, a3t2=8, a4t1=9, a4t2=10, a5t1=11, a5t2=12, a6=14, a7=16)
KINDS = ("core", "y", "q", "p", "w", "x", "t", "fe1", "fy", "f2m", "fe2", "fe3", "out", "loc")
KIND = {name: i for i, name in enumerate(KINDS)}


def kernel(
    a, g, o, abuf, gbuf, acc, sb0, rb0, sby, ry, sbq, rq, sbp, rp, sbw, rw, sbx, rx, sbt, rt, fin,
    keep_p, keep_q, keep_w, asem, gsem, ssem, rsem,
):
    mats, tokens, rows = a.shape[1:]
    ff = g.shape[3]
    nk, nj = tokens // DEPTH, ff // COLS
    blocks = mats * nj
    half, part = rows // 2, rows // 8
    slab = tokens // ASLABS
    per_dot = ASLABS // nk

    me = lax.axis_index("dp")
    c, z, y = me % 2, (me // 2) % 4, me // 8
    mid = (z == 1) | (z == 2)
    end = jnp.logical_not(mid)
    i = z // 2

    def at(y, z, c):
        return (y * 4 + z) * 2 + c

    sib, across = at(y, z, 1 - c), at(1 - y, z, c)
    inner, partner, outer = at(y, 1 + i, c), at(y, 3 - z, c), at(y, i * 3, c)

    def rc(kind, slot, src, dst, dev):
        return pltpu.make_async_remote_copy(
            src_ref=src, dst_ref=dst, send_sem=ssem.at[KIND[kind], slot], recv_sem=rsem.at[KIND[kind], slot],
            device_id={"dp": dev}, device_id_type=MESH,
        )

    def gcopy(s):
        b, k = s // nk, s % nk
        n, j = b // nj, b % nj
        return pltpu.make_async_copy(
            g.at[0, n, pl.ds(pl.multiple_of(k * DEPTH, DEPTH), DEPTH), pl.ds(pl.multiple_of(j * COLS, COLS), COLS)],
            gbuf.at[s % GBUFS], gsem.at[s % GBUFS],
        )

    def acopy(n, s):
        return pltpu.make_async_copy(
            a.at[0, n, pl.ds(pl.multiple_of(s * slab, slab), slab), :],
            abuf.at[n % 2, pl.ds(pl.multiple_of(s * slab, slab), slab), :], asem.at[n % 2, s],
        )

    def piece(first):
        return pl.ds(pl.multiple_of(first * part, part), part)

    def c_core(k):
        s = k % SLOTS
        return rc("core", s, sb0.at[s], rb0.at[s], sib)

    def c_y(k):
        s = k % SLOTS
        return rc("y", s, sby.at[s], ry.at[s], across)

    def c_q(k):
        s = k % SLOTS
        return rc("q", s, sbq.at[s], rq.at[s], inner)

    def c_p(k):
        s = k % SLOTS
        return rc("p", s, sbp.at[s], rp.at[s], inner)

    def c_w(k):
        s = k % SLOTS
        return rc("w", s, sbw.at[s], rw.at[s], partner)

    def c_x(k):
        s = k % SLOTS
        return rc("x", s, sbx.at[s], rx.at[s], partner)

    def c_t(k):
        s = k % SLOTS
        return rc("t", s, sbt.at[s], rt.at[s], across)

    def c_fin(kind, k, which, dev):
        s = k % FSLOTS
        return rc(kind, s, fin.at[s, piece(which), :], fin.at[s, piece(which), :], dev)

    def place(k):
        n, j = k // nj, k % nj
        return o.at[n, pl.ds(pl.multiple_of(c * half, half), half), pl.ds(pl.multiple_of(j * COLS, COLS), COLS)]

    def other_place(k):
        n, j = k // nj, k % nj
        return o.at[n, pl.ds(pl.multiple_of((1 - c) * half, half), half), pl.ds(pl.multiple_of(j * COLS, COLS), COLS)]

    def c_loc(k):
        s = k % FSLOTS
        return pltpu.make_async_copy(fin.at[s], place(k), ssem.at[KIND["loc"], s])

    def c_out(k):
        s = k % FSLOTS
        return rc("out", s, fin.at[s], place(k), sib)

    def c_out_in(k):
        s = k % FSLOTS
        return rc("out", s, fin.at[s], other_place(k), sib)

    def a0(k):
        s = k % SLOTS
        sb0[s] = acc[k % 2, pl.ds(pl.multiple_of((1 - c) * half, half), half), :].astype(BF16)
        c_core(k).start()

    def a1(k):
        s = k % SLOTS
        c_core(k).wait()

        def total(first, count):
            rows_ = pl.ds(pl.multiple_of(c * half + first * part, part), count * part)
            return acc[k % 2, rows_, :] + rb0[s, pl.ds(pl.multiple_of(first * part, part), count * part), :].astype(F32)

        sby[s] = total(1 - y, 1).astype(BF16)
        c_y(k).start()

        @pl.when(end)
        def _():
            sbq[s] = total(2, 2).astype(BF16)
            c_q(k).start()

        @pl.when(mid)
        def _():
            keep_q[s] = total(2, 2)

        keep_p[s] = total(y, 1)

    def a2t1(k):
        s = k % SLOTS
        c_y(k).wait()

        @pl.when(end)
        def _():
            sbp[s] = (keep_p[s] + ry[s].astype(F32)).astype(BF16)
            c_p(k).start()

        @pl.when(mid)
        def _():
            keep_p[s] += ry[s].astype(F32)

    def a2t2(k):
        s = k % SLOTS

        @pl.when(mid)
        def _():
            c_q(k).wait_recv()
            sbw[s] = (keep_q[s, piece(1 - i), :] + rq[s, piece(1 - i), :].astype(F32)).astype(BF16)
            c_w(k).start()
            keep_w[s] = keep_q[s, piece(i), :] + rq[s, piece(i), :].astype(F32)

        @pl.when(end)
        def _():
            c_q(k).wait_send()

    def a3t1(k):
        s = k % SLOTS

        @pl.when(mid)
        def _():
            c_p(k).wait_recv()
            sbx[s] = (keep_p[s] + rp[s].astype(F32)).astype(BF16)
            c_x(k).start()

        @pl.when(end)
        def _():
            c_p(k).wait_send()

    def a3t2(k):
        s = k % SLOTS

        @pl.when(mid)
        def _():
            c_w(k).wait()
            sbt[s] = (keep_w[s] + rw[s].astype(F32)).astype(BF16)
            c_t(k).start()

    def a4t1(k):
        s = k % SLOTS

        @pl.when(mid)
        def _():
            c_x(k).wait()
            fin[k % FSLOTS, piece(y), :] = (sbx[s].astype(F32) + rx[s].astype(F32)).astype(BF16)
            c_fin("fe1", k, y, outer).start()
            c_fin("fy", k, y, across).start()

    def a4t2(k):
        s = k % SLOTS

        @pl.when(mid)
        def _():
            c_t(k).wait()
            fin[k % FSLOTS, piece(2 + i), :] = (sbt[s].astype(F32) + rt[s].astype(F32)).astype(BF16)
            c_fin("f2m", k, 2 + i, partner).start()
            c_fin("fe2", k, 2 + i, outer).start()

    def a5t1(k):
        @pl.when(end)
        def _():
            c_fin("fe1", k, y, outer).wait_recv()
            c_fin("fy", k, y, across).start()

        @pl.when(mid)
        def _():
            c_fin("fe1", k, y, outer).wait_send()

    def a5t2(k):
        @pl.when(mid)
        def _():
            c_fin("f2m", k, 2 + i, partner).wait_send()
            c_fin("f2m", k, 3 - i, partner).wait_recv()
            c_fin("fe3", k, 3 - i, outer).start()

    def a6(k):
        c_fin("fy", k, y, across).wait_send()
        c_fin("fy", k, 1 - y, across).wait_recv()

        @pl.when(end)
        def _():
            c_fin("fe2", k, 2 + i, outer).wait_recv()
            c_fin("fe3", k, 3 - i, outer).wait_recv()

        c_out(k).start()
        c_loc(k).start()

    def a7(k):
        @pl.when(mid)
        def _():
            c_fin("fe2", k, 2 + i, outer).wait_send()
            c_fin("fe3", k, 3 - i, outer).wait_send()

        c_loc(k).wait()
        c_out(k).wait_send()
        c_out_in(k).wait_recv()

    stages = dict(a1=a1, a2t1=a2t1, a2t2=a2t2, a3t1=a3t1, a3t2=a3t2, a4t1=a4t1, a4t2=a4t2, a5t1=a5t1, a5t2=a5t2, a6=a6, a7=a7)

    for k in range(nk):
        for s in range(per_dot):
            acopy(0, k * per_dot + s).start()
        gcopy(k).start()
    for k in range(nk, GBUFS):
        gcopy(k).start()

    barrier = pltpu.get_barrier_semaphore()

    def greet(dev):
        pl.semaphore_signal(barrier, inc=1, device_id={"dp": dev}, device_id_type=MESH)

    greet(sib)
    greet(across)

    @pl.when(mid)
    def _():
        greet(partner)
        greet(outer)
        pl.semaphore_wait(barrier, 4)

    @pl.when(end)
    def _():
        greet(inner)
        pl.semaphore_wait(barrier, 3)

    def step(t, carry):
        n, j = t // nj, t % nj
        for q in range(nk):
            for name in sorted(LAGS, key=LAGS.get, reverse=True):
                lag = LAGS[name]
                if lag % nk == q:
                    k = t - lag // nk

                    @pl.when((k >= 0) & (k < blocks))
                    def _(name=name, k=k):
                        stages[name](k)

            @pl.when(t < blocks)
            def _():
                s = t * nk + q

                @pl.when(j == 0)
                def _():
                    for r in range(per_dot):
                        acopy(n, q * per_dot + r).wait()

                gcopy(s).wait()
                d = lax.dot_general(
                    abuf[n % 2, pl.ds(q * DEPTH, DEPTH), :], gbuf[s % GBUFS], (((0,), (0,)), ((), ())),
                    preferred_element_type=F32,
                )
                if q == 0:
                    acc[t % 2] = d
                else:
                    acc[t % 2] += d

                @pl.when(s + GBUFS < blocks * nk)
                def _():
                    gcopy(s + GBUFS).start()

        @pl.when((j >= 1) & (j <= ASLABS) & (n + 1 < mats))
        def _():
            acopy(n + 1, j - 1).start()

        @pl.when(t < blocks)
        def _():
            a0(t)

        return carry

    lax.fori_loop(0, blocks + max(LAGS.values()) // nk, step, 0)


def solution(mesh):
    def local(a, g):
        _, mats, tokens, rows = a.shape
        ff = g.shape[3]
        nk = tokens // DEPTH
        half, part = rows // 2, rows // 8

        def sent(count):
            return [pltpu.VMEM((SLOTS, count * part, COLS), BF16)] * 2

        return pl.pallas_call(
            kernel,
            out_shape=jax.ShapeDtypeStruct((mats, rows, ff), BF16),
            in_specs=[pl.BlockSpec(memory_space=pl.ANY)] * 2,
            out_specs=pl.BlockSpec(memory_space=pl.ANY),
            scratch_shapes=[
                pltpu.VMEM((2, tokens, rows), BF16),
                pltpu.VMEM((GBUFS, DEPTH, COLS), BF16),
                pltpu.VMEM((2, rows, COLS), F32),
                *sent(4), *sent(1), *sent(2), *sent(1), *sent(1), *sent(1), *sent(1),
                pltpu.VMEM((FSLOTS, half, COLS), BF16),
                pltpu.VMEM((SLOTS, part, COLS), F32),
                pltpu.VMEM((SLOTS, 2 * part, COLS), F32),
                pltpu.VMEM((SLOTS, part, COLS), F32),
                pltpu.SemaphoreType.DMA((2, ASLABS)),
                pltpu.SemaphoreType.DMA((GBUFS,)),
                pltpu.SemaphoreType.DMA((len(KINDS), FSLOTS)),
                pltpu.SemaphoreType.DMA((len(KINDS), FSLOTS)),
            ],
            compiler_params=pltpu.CompilerParams(
                collective_id=0, has_side_effects=True, vmem_limit_bytes=63 * 2**20
            ),
            cost_estimate=pl.CostEstimate(
                flops=2 * mats * tokens * rows * ff, bytes_accessed=2 * mats * tokens * (rows + ff), transcendentals=0
            ),
        )(a, g)

    group = P(("rep", "dp"))
    return jax.shard_map(local, mesh=mesh, in_specs=(group, group), out_specs=P("rep"), check_vma=False)
```

```python
import jax
import jax.numpy as jnp
from jax import lax
from jax.experimental import pallas as pl
from jax.experimental.pallas import tpu as pltpu
from jax.sharding import PartitionSpec as P

MESH = pl.DeviceIdType.MESH
F32, BF16 = jnp.float32, jnp.bfloat16

COLS = 256
DEPTH = 4096
GBUFS = 3
ASLABS = 8
SLOTS = 4
FSLOTS = 8
LAGS = dict(a1=3, a2t1=5, a2t2=6, a3t1=7, a3t2=8, a4t1=9, a4t2=10, a5t1=11, a5t2=12, a6=14, a7=16)
KINDS = ("core", "y", "qf", "qk", "p", "w", "x", "t", "fe1", "fy", "f2m", "fe2", "fe3", "out")
KIND = {name: i for i, name in enumerate(KINDS)}


def kernel(
    a, g, o, abuf, gbuf, acc, sb0, rb0, sby, ry, sbq, rq, sbp, rp, sbw, rw, sbx, rx, sbt, rt,
    keep_p, keep_q, asem, gsem, ssem, rsem,
):
    mats, tokens, rows = a.shape[1:]
    ff = g.shape[3]
    nk, nj = tokens // DEPTH, ff // COLS
    blocks = mats * nj
    half, part = rows // 2, rows // 8
    slab = tokens // ASLABS
    per_dot = ASLABS // nk

    me = lax.axis_index("dp")
    c, z, y = me % 2, (me // 2) % 4, me // 8
    mid = (z == 1) | (z == 2)
    end = jnp.logical_not(mid)
    i = z // 2

    def at(y, z, c):
        return (y * 4 + z) * 2 + c

    sib, across = at(y, z, 1 - c), at(1 - y, z, c)
    inner, partner, outer = at(y, 1 + i, c), at(y, 3 - z, c), at(y, i * 3, c)

    def rc(kind, slot, src, dst, dev):
        return pltpu.make_async_remote_copy(
            src_ref=src, dst_ref=dst, send_sem=ssem.at[KIND[kind], slot], recv_sem=rsem.at[KIND[kind], slot],
            device_id={"dp": dev}, device_id_type=MESH,
        )

    def gcopy(s):
        b, k = s // nk, s % nk
        n, j = b // nj, b % nj
        return pltpu.make_async_copy(
            g.at[0, n, pl.ds(pl.multiple_of(k * DEPTH, DEPTH), DEPTH), pl.ds(pl.multiple_of(j * COLS, COLS), COLS)],
            gbuf.at[s % GBUFS], gsem.at[s % GBUFS],
        )

    def acopy(n, s):
        return pltpu.make_async_copy(
            a.at[0, n, pl.ds(pl.multiple_of(s * slab, slab), slab), :],
            abuf.at[n % 2, pl.ds(pl.multiple_of(s * slab, slab), slab), :], asem.at[n % 2, s],
        )

    def piece(first):
        return pl.ds(pl.multiple_of(first * part, part), part)

    def c_core(k):
        s = k % SLOTS
        return rc("core", s, sb0.at[s], rb0.at[s], sib)

    def c_y(k):
        s = k % SLOTS
        return rc("y", s, sby.at[s], ry.at[s], across)

    def c_q(k, which, kind):
        s = k % SLOTS
        return rc(kind, s, sbq.at[s, piece(which), :], rq.at[s, piece(which), :], inner)

    def c_p(k):
        s = k % SLOTS
        return rc("p", s, sbp.at[s], rp.at[s], inner)

    def c_w(k):
        s = k % SLOTS
        return rc("w", s, sbw.at[s], rw.at[s], partner)

    def c_x(k):
        s = k % SLOTS
        return rc("x", s, sbx.at[s], rx.at[s], partner)

    def c_t(k):
        s = k % SLOTS
        return rc("t", s, sbt.at[s], rt.at[s], across)

    def place(k, first, count):
        n, j = k // nj, k % nj
        return n, pl.ds(pl.multiple_of(first * part, part), count * part), pl.ds(pl.multiple_of(j * COLS, COLS), COLS)

    def c_fin(kind, k, which, dev):
        at_ = o.at[place(k, 4 * c + which, 1)]
        return rc(kind, k % FSLOTS, at_, at_, dev)

    def c_out(k, core):
        at_ = o.at[place(k, 4 * core, 4)]
        return rc("out", k % FSLOTS, at_, at_, sib)

    def a0(k):
        s = k % SLOTS
        sb0[s] = acc[k % 2, pl.ds(pl.multiple_of((1 - c) * half, half), half), :].astype(BF16)
        c_core(k).start()

    def a1(k):
        s = k % SLOTS
        c_core(k).wait()

        def total(first, count):
            rows_ = pl.ds(pl.multiple_of(c * half + first * part, part), count * part)
            return acc[k % 2, rows_, :] + rb0[s, pl.ds(pl.multiple_of(first * part, part), count * part), :].astype(F32)

        sby[s] = total(1 - y, 1).astype(BF16)
        c_y(k).start()

        @pl.when(end)
        def _():
            sbq[s] = total(2, 2).astype(BF16)
            c_q(k, 1 - i, "qf").start()
            c_q(k, i, "qk").start()

        @pl.when(mid)
        def _():
            keep_q[s] = total(2, 2)

        keep_p[s] = total(y, 1)

    def a2t1(k):
        s = k % SLOTS
        c_y(k).wait()

        @pl.when(end)
        def _():
            sbp[s] = (keep_p[s] + ry[s].astype(F32)).astype(BF16)
            c_p(k).start()

        @pl.when(mid)
        def _():
            keep_p[s] += ry[s].astype(F32)

    def a2t2(k):
        s = k % SLOTS

        @pl.when(mid)
        def _():
            c_q(k, 1 - i, "qf").wait_recv()
            sbw[s] = (keep_q[s, piece(1 - i), :] + rq[s, piece(1 - i), :].astype(F32)).astype(BF16)
            c_w(k).start()

        @pl.when(end)
        def _():
            c_q(k, 1 - i, "qf").wait_send()
            c_q(k, i, "qk").wait_send()

    def a3t1(k):
        s = k % SLOTS

        @pl.when(mid)
        def _():
            c_p(k).wait_recv()
            sbx[s] = (keep_p[s] + rp[s].astype(F32)).astype(BF16)
            c_x(k).start()

        @pl.when(end)
        def _():
            c_p(k).wait_send()

    def a3t2(k):
        s = k % SLOTS

        @pl.when(mid)
        def _():
            c_w(k).wait()
            c_q(k, i, "qk").wait_recv()
            sbt[s] = (keep_q[s, piece(i), :] + rq[s, piece(i), :].astype(F32) + rw[s].astype(F32)).astype(BF16)
            c_t(k).start()

    def a4t1(k):
        s = k % SLOTS

        @pl.when(mid)
        def _():
            c_x(k).wait()
            o[place(k, 4 * c + y, 1)] = (sbx[s].astype(F32) + rx[s].astype(F32)).astype(BF16)
            c_fin("fe1", k, y, outer).start()
            c_fin("fy", k, y, across).start()

    def a4t2(k):
        s = k % SLOTS

        @pl.when(mid)
        def _():
            c_t(k).wait()
            o[place(k, 4 * c + 2 + i, 1)] = (sbt[s].astype(F32) + rt[s].astype(F32)).astype(BF16)
            c_fin("f2m", k, 2 + i, partner).start()
            c_fin("fe2", k, 2 + i, outer).start()

    def a5t1(k):
        @pl.when(end)
        def _():
            c_fin("fe1", k, y, outer).wait_recv()
            c_fin("fy", k, y, across).start()

        @pl.when(mid)
        def _():
            c_fin("fe1", k, y, outer).wait_send()

    def a5t2(k):
        @pl.when(mid)
        def _():
            c_fin("f2m", k, 2 + i, partner).wait_send()
            c_fin("f2m", k, 3 - i, partner).wait_recv()
            c_fin("fe3", k, 3 - i, outer).start()

    def a6(k):
        c_fin("fy", k, y, across).wait_send()
        c_fin("fy", k, 1 - y, across).wait_recv()

        @pl.when(end)
        def _():
            c_fin("fe2", k, 2 + i, outer).wait_recv()
            c_fin("fe3", k, 3 - i, outer).wait_recv()

        c_out(k, c).start()

    def a7(k):
        @pl.when(mid)
        def _():
            c_fin("fe2", k, 2 + i, outer).wait_send()
            c_fin("fe3", k, 3 - i, outer).wait_send()

        c_out(k, c).wait_send()
        c_out(k, 1 - c).wait_recv()

    stages = dict(a1=a1, a2t1=a2t1, a2t2=a2t2, a3t1=a3t1, a3t2=a3t2, a4t1=a4t1, a4t2=a4t2, a5t1=a5t1, a5t2=a5t2, a6=a6, a7=a7)

    for k in range(nk):
        for s in range(per_dot):
            acopy(0, k * per_dot + s).start()
        if k < GBUFS:
            gcopy(k).start()
    for k in range(nk, GBUFS):
        gcopy(k).start()

    barrier = pltpu.get_barrier_semaphore()

    def greet(dev):
        pl.semaphore_signal(barrier, inc=1, device_id={"dp": dev}, device_id_type=MESH)

    greet(sib)
    greet(across)

    @pl.when(mid)
    def _():
        greet(partner)
        greet(outer)
        pl.semaphore_wait(barrier, 4)

    @pl.when(end)
    def _():
        greet(inner)
        pl.semaphore_wait(barrier, 3)

    def step(t, carry):
        n, j = t // nj, t % nj
        for q in range(nk):
            for name in sorted(LAGS, key=LAGS.get, reverse=True):
                lag = LAGS[name]
                if lag % nk == q:
                    k = t - lag // nk

                    @pl.when((k >= 0) & (k < blocks))
                    def _(name=name, k=k):
                        stages[name](k)

            @pl.when(t < blocks)
            def _():
                s = t * nk + q

                @pl.when(j == 0)
                def _():
                    for r in range(per_dot):
                        acopy(n, q * per_dot + r).wait()

                gcopy(s).wait()
                d = lax.dot_general(
                    abuf[n % 2, pl.ds(q * DEPTH, DEPTH), :], gbuf[s % GBUFS], (((0,), (0,)), ((), ())),
                    preferred_element_type=F32,
                )
                if q == 0:
                    acc[t % 2] = d
                else:
                    acc[t % 2] += d

                @pl.when(s + GBUFS < blocks * nk)
                def _():
                    gcopy(s + GBUFS).start()

        @pl.when((j >= 1) & (j <= ASLABS) & (n + 1 < mats))
        def _():
            acopy(n + 1, j - 1).start()

        @pl.when(t < blocks)
        def _():
            a0(t)

        return carry

    lax.fori_loop(0, blocks + max(LAGS.values()) // nk, step, 0)


def solution(mesh):
    def local(a, g):
        _, mats, tokens, rows = a.shape
        ff = g.shape[3]
        part = rows // 8

        def sent(count):
            return [pltpu.VMEM((SLOTS, count * part, COLS), BF16)] * 2

        return pl.pallas_call(
            kernel,
            out_shape=pltpu.VMEM((mats, rows, ff), BF16),
            in_specs=[pl.BlockSpec(memory_space=pl.ANY)] * 2,
            out_specs=pl.BlockSpec(memory_space=pltpu.VMEM),
            scratch_shapes=[
                pltpu.VMEM((2, tokens, rows), BF16),
                pltpu.VMEM((GBUFS, DEPTH, COLS), BF16),
                pltpu.VMEM((2, rows, COLS), F32),
                *sent(4), *sent(1), *sent(2), *sent(1), *sent(1), *sent(1), *sent(1),
                pltpu.VMEM((SLOTS, part, COLS), F32),
                pltpu.VMEM((SLOTS, 2 * part, COLS), F32),
                pltpu.SemaphoreType.DMA((2, ASLABS)),
                pltpu.SemaphoreType.DMA((GBUFS,)),
                pltpu.SemaphoreType.DMA((len(KINDS), FSLOTS)),
                pltpu.SemaphoreType.DMA((len(KINDS), FSLOTS)),
            ],
            compiler_params=pltpu.CompilerParams(
                collective_id=0, has_side_effects=True, vmem_limit_bytes=45 * 2**20
            ),
            cost_estimate=pl.CostEstimate(
                flops=2 * mats * tokens * rows * ff, bytes_accessed=2 * mats * tokens * (rows + ff), transcendentals=0
            ),
        )(a, g)

    group = P(("rep", "dp"))
    return jax.shard_map(local, mesh=mesh, in_specs=(group, group), out_specs=P("rep"), check_vma=False)
```
